256 devices in a mesh: dp: 2 (over z_hi), group: 16 (over x, y), seq: 8 (over z_lo, core).
Axes of the slice: x: 4, y: 4, z: 8 (z_hi: 2, z_lo: 4; z = z_hi * 4 + z_lo), core: 2. Of those that a mesh axis runs over, the one named last changes fastest.
Arguments:
- queries: bfloat16 [2, 4096, 2560], P('dp', 'group', 'seq'), may hold values from -6 to 6
- keys: bfloat16 [2, 4096, 2560], P('dp', 'group', 'seq'), may hold values from -6 to 6
- values: bfloat16 [2, 4096, 2560], P('dp', 'group', 'seq'), may hold values from -6 to 6
- cotangent: bfloat16 [2, 4096, 2560], P('dp', 'group', 'seq'), may hold values from -18 to 18
- level_bias: float32 [3, 40], P(None, 'seq'), may hold values from -3 to 3
- off_mid: int32 [40], P('seq'), may hold values from 0 to 7
- off_far: int32 [40], P('seq'), may hold values from 0 to 63
Outputs:
- attended: bfloat16 [2, 4096, 2560], P('dp', 'group', 'seq')
- query_grad: bfloat16 [2, 4096, 2560], P('dp', 'group', 'seq')
- key_grad: bfloat16 [2, 4096, 2560], P('dp', 'group', 'seq')
- value_grad: bfloat16 [2, 4096, 2560], P('dp', 'group', 'seq')
- bias_grad: float32 [3, 40], replicated
The draws below stay inside these ranges and needn't reach their ends.
All inputs are finite; a program needn't handle non-finite values.
Results may differ from the reference program's by a relative error of at most 0.04.
Values may be sent and summed in bfloat16 or wider, within the bound.
No kernel may reach another device: no remote copies, remote signals or barrier semaphores. Data moves between devices by JAX's collectives and lax.ppermute only.
A program may use at most 64 MiB of HBM per device.

```python
import math
import jax
import jax.numpy as jnp
from jax import lax

D = 2560
HEADS = 40
HD = 64
SEG_NEAR = 256
R_MID = 8
R_FAR = 64
BATCH = 2
TOKENS = 4096
SEG_MID = 4096


def level_offsets(key):
    base = jax.random.fold_in(key, 101)
    middle = jax.random.randint(jax.random.fold_in(base, 1), (HEADS,), 0, R_MID)
    farther = jax.random.randint(jax.random.fold_in(base, 2), (HEADS,), 0, R_FAR)
    return (middle.astype(jnp.int32), farther.astype(jnp.int32))


def drawn_draw(key, salt):
    noise_key = jax.random.fold_in(key, salt)
    shape = (BATCH, TOKENS, HEADS, HD)
    base = jnp.clip(jax.random.normal(noise_key, shape, jnp.float32), -6.0, 6.0)
    return base.reshape(BATCH, TOKENS, D).astype(jnp.bfloat16)


def draw_queries(key, part):
    return drawn_draw(key, 11)


def draw_keys(key, part):
    return drawn_draw(key, 12)


def draw_cotangent(key, part):
    noise_key = jax.random.fold_in(key, 31)
    position = jnp.arange(TOKENS, dtype=jnp.float32)
    rising = 1.0 + 2.0 * position / TOKENS
    base = jnp.clip(jax.random.normal(noise_key, (BATCH, TOKENS, D), jnp.float32), -6.0, 6.0)
    return (base * rising[None, :, None]).astype(jnp.bfloat16)


def draw_off_mid(key, part):
    return level_offsets(key)[0]


def draw_off_far(key, part):
    return level_offsets(key)[1]


def block_scale(own_key, extent, split, low, top_value):
    loudness, own = 1.0, jax.random.fold_in(own_key, 6)
    for axis_at, shards_of in split:
        draws = jnp.exp(jax.random.uniform(jax.random.fold_in(own, axis_at), (shards_of,), jnp.float32, low / len(split), top_value / len(split)))
        loudness = loudness * jnp.repeat(draws, extent[axis_at] // shards_of).reshape([-1 if axis == axis_at else 1 for axis in range(len(extent))])
    return loudness


def bell_draw(key, extent, deviation, reach, shards=(), kind=jnp.bfloat16):
    entries = deviation * jax.random.normal(key, extent, jnp.float32)
    if shards:
        entries = entries * block_scale(key, extent, shards, -0.22, 0.18)
    return jnp.clip(entries, -reach, reach).astype(kind)


def setup_inputs(seed: int = 0) -> dict:
    arg_keys = jax.random.split(jax.random.key(seed), 8)
    return {
        "queries": draw_queries(jax.random.fold_in(arg_keys[7], 71), 0),
        "keys": draw_keys(jax.random.fold_in(arg_keys[7], 71), 0),
        "values": bell_draw(arg_keys[2], (BATCH, TOKENS, D), 1.0, 6.0, ((0, 2), (1, 16), (2, 8))),
        "cotangent": draw_cotangent(jax.random.fold_in(arg_keys[7], 71), 0),
        "level_bias": bell_draw(arg_keys[4], (3, HEADS), 1.0, 3.0, ((1, 8),), jnp.float32),
        "off_mid": draw_off_mid(jax.random.fold_in(arg_keys[7], 71), 0),
        "off_far": draw_off_far(jax.random.fold_in(arg_keys[7], 71), 0),
    }


def product(form, left, right):
    return jnp.einsum(form, left.astype(jnp.float32), right.astype(jnp.float32))

def select_rows(source, stride, offsets):
    count = source.shape[0] // stride
    shaped = source.reshape((count, stride) + source.shape[1:])
    picker = offsets.astype(jnp.int32).reshape((1, 1, -1) + (1,) * (source.ndim - 2))
    picker = jnp.broadcast_to(picker, (count, 1) + source.shape[1:])
    return jnp.take_along_axis(shaped, picker, axis=1)[:, 0]

def place_rows(source, stride, offsets, filler):
    heads = source.shape[1]
    marked = jnp.arange(stride, dtype=jnp.int32)[:, None] == offsets.astype(jnp.int32)[None, :]
    marked = marked.reshape((1, stride, heads) + (1,) * (source.ndim - 2))
    spread = jnp.where(marked, source[:, None], jnp.asarray(filler, source.dtype))
    return spread.reshape((source.shape[0] * stride,) + source.shape[1:])

def forward_level(queries, keys, values, visible, scaling):
    scores = product('qhe,khe->hqk', queries, keys) * scaling
    scores = jnp.where(visible[None], scores, -jnp.inf)
    highest = lax.optimization_barrier(jnp.max(scores, axis=2, keepdims=True))
    log_sum = highest + jnp.log(lax.optimization_barrier(jnp.sum(jnp.exp(scores - highest), axis=2, keepdims=True)))
    weights = jnp.exp(scores - log_sum).astype(jnp.bfloat16)
    return (log_sum[:, :, 0].T, product('hqk,khe->qhe', weights, values))

def backward_level(queries, keys, values, cotangent, visible, log_total, row_delta, bias_row, scaling):
    scores = product('qhe,khe->hqk', queries, keys) * scaling
    shifted = scores + bias_row[:, None, None] - log_total.T[:, :, None]
    weight = jnp.where(visible[None], jnp.exp(jnp.where(visible[None], shifted, 0.0)), 0.0)
    inner = product('qhe,khe->hqk', cotangent, values)
    dscore = weight * (inner - row_delta.T[:, :, None])
    dscore_low = dscore.astype(jnp.bfloat16)
    weight_low = weight.astype(jnp.bfloat16)
    return (product('hqk,khe->qhe', dscore_low, keys), product('hqk,qhe->khe', dscore_low, queries), product('hqk,qhe->khe', weight_low, cotangent))

def causal_forward(queries, keys, values, scaling):
    length = queries.shape[0]
    block_rows = min(128, length)
    lse_parts = []
    out_parts = []
    for first_row in range(0, length, block_rows):
        last_row = first_row + block_rows
        query_place = jnp.arange(first_row, last_row, dtype=jnp.int32)
        key_place = jnp.arange(last_row, dtype=jnp.int32)
        visible = key_place[None, :] <= query_place[:, None]
        block_lse, block_out = forward_level(queries[first_row:last_row], keys[:last_row], values[:last_row], visible, scaling)
        lse_parts.append(block_lse)
        out_parts.append(block_out)
    return (jnp.concatenate(lse_parts, 0), jnp.concatenate(out_parts, 0))

def causal_backward(queries, keys, values, cotangent, log_total, row_delta, bias_row, scaling):
    length = queries.shape[0]
    block_rows = min(128, length)
    query_parts = []
    key_total = jnp.zeros(keys.shape, jnp.float32)
    value_total = jnp.zeros(values.shape, jnp.float32)
    for first_row in range(0, length, block_rows):
        last_row = first_row + block_rows
        query_place = jnp.arange(first_row, last_row, dtype=jnp.int32)
        key_place = jnp.arange(last_row, dtype=jnp.int32)
        visible = key_place[None, :] <= query_place[:, None]
        part_q, part_k, part_v = backward_level(queries[first_row:last_row], keys[:last_row], values[:last_row], cotangent[first_row:last_row], visible, log_total[first_row:last_row], row_delta[first_row:last_row], bias_row, scaling)
        query_parts.append(part_q)
        padding = ((0, length - last_row), (0, 0), (0, 0))
        key_total = key_total + jnp.pad(part_k, padding)
        value_total = value_total + jnp.pad(part_v, padding)
    return (jnp.concatenate(query_parts, 0), key_total, value_total)

def split_rows(source, length):
    return source.reshape((source.shape[0] // length, length) + source.shape[1:])

def join_rows(source):
    return source.reshape((source.shape[0] * source.shape[1],) + source.shape[2:])

def one_sequence(query_rows, key_rows, value_rows, grad_rows, level_bias, off_mid, off_far):
    scaling = HD ** (-0.5)
    mid_length = SEG_MID // R_MID

    def near_forward(items):
        return causal_forward(items[0], items[1], items[2], scaling)
    near_lse, near_out = lax.map(near_forward, (split_rows(query_rows, SEG_NEAR), split_rows(key_rows, SEG_NEAR), split_rows(value_rows, SEG_NEAR)))
    near_lse = join_rows(near_lse)
    near_out = join_rows(near_out)
    mid_queries = select_rows(query_rows, R_MID, off_mid)
    mid_keys = select_rows(key_rows, R_MID, off_mid)
    mid_values = select_rows(value_rows, R_MID, off_mid)
    mid_lse, mid_out = lax.map(near_forward, (split_rows(mid_queries, mid_length), split_rows(mid_keys, mid_length), split_rows(mid_values, mid_length)))
    mid_lse = join_rows(mid_lse)
    mid_out = join_rows(mid_out)
    far_queries = select_rows(query_rows, R_FAR, off_far)
    far_keys = select_rows(key_rows, R_FAR, off_far)
    far_values = select_rows(value_rows, R_FAR, off_far)
    far_lse, far_out = causal_forward(far_queries, far_keys, far_values, scaling)
    gate_near = near_lse + level_bias[0][None, :]
    gate_mid = place_rows(mid_lse, R_MID, off_mid, -jnp.inf) + level_bias[1][None, :]
    gate_far = place_rows(far_lse, R_FAR, off_far, -jnp.inf) + level_bias[2][None, :]
    highest = jnp.maximum(gate_near, jnp.maximum(gate_mid, gate_far))
    log_total = highest + jnp.log(jnp.exp(gate_near - highest) + jnp.exp(gate_mid - highest) + jnp.exp(gate_far - highest))
    share_near = jnp.exp(gate_near - log_total)
    share_mid = jnp.exp(gate_mid - log_total)
    share_far = jnp.exp(gate_far - log_total)
    mid_full = place_rows(mid_out, R_MID, off_mid, 0.0)
    far_full = place_rows(far_out, R_FAR, off_far, 0.0)
    mixed = share_near[..., None] * near_out + share_mid[..., None] * mid_full + share_far[..., None] * far_full
    attended = mixed.astype(jnp.bfloat16)
    grad_float = grad_rows.astype(jnp.float32)
    row_delta = lax.optimization_barrier(jnp.sum(grad_float * attended.astype(jnp.float32), axis=2))
    level_terms = jnp.stack([lax.optimization_barrier(jnp.sum(share_near * (lax.optimization_barrier(jnp.sum(grad_float * near_out, axis=2)) - row_delta), axis=0)), lax.optimization_barrier(jnp.sum(share_mid * (lax.optimization_barrier(jnp.sum(grad_float * mid_full, axis=2)) - row_delta), axis=0)), lax.optimization_barrier(jnp.sum(share_far * (lax.optimization_barrier(jnp.sum(grad_float * far_full, axis=2)) - row_delta), axis=0))])

    def near_backward(items):
        return causal_backward(items[0], items[1], items[2], items[3], items[4], items[5], level_bias[0], scaling)
    near_dq, near_dk, near_dv = lax.map(near_backward, (split_rows(query_rows, SEG_NEAR), split_rows(key_rows, SEG_NEAR), split_rows(value_rows, SEG_NEAR), split_rows(grad_rows, SEG_NEAR), split_rows(log_total, SEG_NEAR), split_rows(row_delta, SEG_NEAR)))
    near_dq = join_rows(near_dq)
    near_dk = join_rows(near_dk)
    near_dv = join_rows(near_dv)
    mid_grads = select_rows(grad_rows, R_MID, off_mid)
    mid_total = select_rows(log_total, R_MID, off_mid)
    mid_delta = select_rows(row_delta, R_MID, off_mid)

    def mid_backward(items):
        return causal_backward(items[0], items[1], items[2], items[3], items[4], items[5], level_bias[1], scaling)
    mid_dq, mid_dk, mid_dv = lax.map(mid_backward, (split_rows(mid_queries, mid_length), split_rows(mid_keys, mid_length), split_rows(mid_values, mid_length), split_rows(mid_grads, mid_length), split_rows(mid_total, mid_length), split_rows(mid_delta, mid_length)))
    mid_dq = join_rows(mid_dq)
    mid_dk = join_rows(mid_dk)
    mid_dv = join_rows(mid_dv)
    far_grads = select_rows(grad_rows, R_FAR, off_far)
    far_total = select_rows(log_total, R_FAR, off_far)
    far_delta = select_rows(row_delta, R_FAR, off_far)
    far_dq, far_dk, far_dv = causal_backward(far_queries, far_keys, far_values, far_grads, far_total, far_delta, level_bias[2], scaling)
    query_grad = scaling * (near_dq + place_rows(mid_dq, R_MID, off_mid, 0.0) + place_rows(far_dq, R_FAR, off_far, 0.0))
    key_grad = scaling * (near_dk + place_rows(mid_dk, R_MID, off_mid, 0.0) + place_rows(far_dk, R_FAR, off_far, 0.0))
    value_grad = near_dv + place_rows(mid_dv, R_MID, off_mid, 0.0) + place_rows(far_dv, R_FAR, off_far, 0.0)
    return (attended.reshape(TOKENS, D), query_grad.astype(jnp.bfloat16).reshape(TOKENS, D), key_grad.astype(jnp.bfloat16).reshape(TOKENS, D), value_grad.astype(jnp.bfloat16).reshape(TOKENS, D), level_terms)

def reference(queries, keys, values, cotangent, level_bias, off_mid, off_far):
    shape_rows = (TOKENS, HEADS, HD)
    results = [one_sequence(queries[member].reshape(shape_rows), keys[member].reshape(shape_rows), values[member].reshape(shape_rows), cotangent[member].reshape(shape_rows), level_bias, off_mid, off_far) for member in range(BATCH)]
    attended = jnp.stack([result[0] for result in results])
    query_grad = jnp.stack([result[1] for result in results])
    key_grad = jnp.stack([result[2] for result in results])
    value_grad = jnp.stack([result[3] for result in results])
    bias_grad = lax.optimization_barrier(jnp.sum(jnp.stack([result[4] for result in results]), axis=0)) / math.sqrt(BATCH * TOKENS)
    return (attended, query_grad, key_grad, value_grad, bias_grad)
```

```python
import functools
import math

import jax
import jax.numpy as jnp
from jax import lax
from jax.experimental import pallas as pl
from jax.experimental.pallas import tpu as pltpu
from jax.sharding import Mesh
from jax.sharding import PartitionSpec as P

HD = 64
R_MID = 8
R_FAR = 64
GROUP = ("group_0", "group_1")
SEQ = ("seq_0", "seq_1")
DP_SEQ = ("dp", "seq_0", "seq_1")

ROWS = 40
COLS = 384
MID_ROWS = 32
FAR_ROWS = 4
SUM_ROW = MID_ROWS + FAR_ROWS
STRIDE = 3
STAT = 5 * HD
BACK_STAT = 4 * HD
HIDDEN = -1e30
FAR_AWAY = 1 << 20

BF16 = jnp.bfloat16
F32 = jnp.float32


def dot(left, right, left_dim=1, right_dim=0):
    return lax.dot_general(
        left, right, (((left_dim,), (right_dim,)), ((), ())), preferred_element_type=F32
    )


def three_parts(x):
    high = x.astype(BF16).astype(F32)
    middle = (x - high).astype(BF16).astype(F32)
    return high, middle, x - high - middle


def whole_sum(x):
    return jnp.sum(jnp.sum(x, axis=0, keepdims=True), axis=1, keepdims=True)


def stacked(parts, count, width):
    row = lax.broadcasted_iota(jnp.int32, (count, width), 0)
    block = jnp.zeros((count, width), F32)
    for n, part in enumerate(parts):
        block = jnp.where(row == n, part, block)
    return block


def row_places(place, mid, far):
    nested = lax.rem(far, R_MID) == mid
    in_mid = place < MID_ROWS
    in_far = jnp.logical_and(place >= MID_ROWS, place < SUM_ROW)
    in_far = jnp.logical_and(in_far, jnp.logical_not(nested))
    at = jnp.where(in_mid, place * R_MID + mid, (place - MID_ROWS) * R_FAR + far)
    return at, in_mid, in_far, nested


def picker(tok, mid, far):
    place = lax.broadcasted_iota(jnp.int32, (ROWS, tok), 0)
    token = lax.broadcasted_iota(jnp.int32, (ROWS, tok), 1)
    at, in_mid, in_far, _ = row_places(place, mid, far)
    hit = jnp.logical_and(jnp.logical_or(in_mid, in_far), at == token)
    return jnp.where(hit, 1.0, 0.0).astype(BF16)


def dilated(tok, mid, far):
    token = lax.broadcasted_iota(jnp.int32, (1, tok), 1)
    in_mid = jnp.bitwise_and(token, R_MID - 1) == mid
    in_far = jnp.bitwise_and(token, R_FAR - 1) == far
    return jnp.logical_or(in_mid, in_far)


def causal(tok):
    key_at = lax.broadcasted_iota(jnp.int32, (tok, tok), 0)
    query_at = lax.broadcasted_iota(jnp.int32, (tok, tok), 1)
    return key_at <= query_at


def near_forward_kernel(
    mid_ref, far_ref, q_ref, k_ref, v_ref, c_ref, send_ref, stat_ref, att_ref
):
    tok = q_ref.shape[2]
    heads = q_ref.shape[1] // HD
    scale = HD**-0.5
    visible = causal(tok)
    place = lax.broadcasted_iota(jnp.int32, (ROWS, HD), 0)
    lane = lax.broadcasted_iota(jnp.int32, (ROWS, HD), 1)
    lses, deltas = [], []
    for h in range(heads):
        mid, far = mid_ref[h], far_ref[h]
        own = slice(h * HD, (h + 1) * HD)
        q, k, v, c = (ref[0, own, :] for ref in (q_ref, k_ref, v_ref, c_ref))
        s = jnp.where(visible, dot(k, q, 0, 0) * scale, HIDDEN)
        top = jnp.max(s, axis=0, keepdims=True)
        p = jnp.exp(s - top)
        size = jnp.sum(p, axis=0, keepdims=True)
        lse = top + jnp.log(size)
        out = dot(v, p.astype(BF16)) * (1.0 / size)
        out_low = out.astype(BF16)
        att_ref[own, :] = out_low
        c32 = c.astype(F32)
        out_round = out_low.astype(F32)
        lses.append(lse)
        deltas.append(jnp.sum(c32 * out_round, axis=0, keepdims=True))
        rest = jnp.sum(c32 * (out - out_round), axis=0, keepdims=True)
        rest = jnp.where(dilated(tok, mid, far), 0.0, rest)
        rest = jnp.sum(rest, axis=1, keepdims=True)
        stats = stacked(three_parts(lse), HD, tok).astype(BF16)
        pieces = jnp.concatenate([q, k, v, c, out_low, stats], axis=0)
        block = dot(picker(tok, mid, far), pieces, 1, 1)
        send_ref[h * STRIDE, :, 0:STAT] = block[:, 0:STAT].astype(BF16)
        row = jnp.zeros((1, HD), F32)
        for n, part in enumerate(three_parts(rest)):
            row = jnp.where(lane[0:1] == n, part, row)
        last = jnp.where(place == SUM_ROW, row, block[:, STAT : STAT + HD])
        send_ref[h * STRIDE, :, STAT : STAT + HD] = last.astype(BF16)
    stat_ref[...] = stacked(lses + [lses[0]] * (8 - heads) + deltas, 16, tok)


def near_backward_kernel(
    mid_ref, far_ref, q_ref, k_ref, v_ref, c_ref, stat_ref, dq_ref, dk_ref, dv_ref
):
    tok = q_ref.shape[2]
    heads = q_ref.shape[1] // HD
    scale = HD**-0.5
    visible = causal(tok)
    for h in range(heads):
        own = slice(h * HD, (h + 1) * HD)
        q, k, v, c = (ref[0, own, :] for ref in (q_ref, k_ref, v_ref, c_ref))
        lse = stat_ref[h : h + 1, :]
        delta = stat_ref[8 + h : 9 + h, :]
        lse = jnp.where(dilated(tok, mid_ref[h], far_ref[h]), -HIDDEN, lse)
        s = jnp.where(visible, dot(k, q, 0, 0) * scale, HIDDEN)
        weight = jnp.exp(s - lse)
        dscore = (weight * (dot(v, c, 0, 0) - delta)).astype(BF16)
        weight = weight.astype(BF16)
        dq_ref[own, :] = dot(k, dscore)
        dk_ref[own, :] = dot(q, dscore, 1, 1)
        dv_ref[own, :] = dot(c, weight, 1, 1)


def far_kernel(
    mid_ref, far_ref, bias_ref, x_ref, y_ref, turned_ref, one_ref, two_ref, dk_ref, dv_ref
):
    total_rows = x_ref.shape[0]
    heads = mid_ref.shape[0]
    scale = HD**-0.5
    head = jnp.minimum(lax.axis_index(GROUP) // STRIDE, heads - 1)
    column = lax.axis_index(SEQ) * heads + head
    mid, far = mid_ref[head], far_ref[head]
    tok = MID_ROWS * R_MID
    b0, b1, b2 = bias_ref[0, head], bias_ref[1, head], bias_ref[2, head]
    e1 = jnp.exp(jnp.full((1, 1), b1, F32))
    e2 = jnp.exp(jnp.full((1, 1), b2, F32))
    per = 128

    def codes(row):
        slab = jnp.right_shift(row * 1639, 16)
        place = row - slab * ROWS
        at, in_mid, in_far, nested = row_places(place, mid, far)
        at = at + slab * tok
        also = jnp.logical_and(in_mid, jnp.bitwise_and(at, R_FAR - 1) == far)
        in_far = jnp.logical_or(in_far, jnp.logical_and(also, nested))
        return at, in_mid, in_far, place

    key_at, key_mid, key_far, _ = codes(lax.broadcasted_iota(jnp.int32, (total_rows, per), 0))
    one_ref[...] = jnp.where(key_mid, key_at, FAR_AWAY)
    two_ref[...] = jnp.where(key_far, key_at, FAR_AWAY)
    dk_ref[...] = jnp.zeros_like(dk_ref)
    dv_ref[...] = jnp.zeros_like(dv_ref)
    zero = jnp.zeros((1, 1), F32)
    sums = [zero, zero, zero]
    for first in range(0, total_rows, per):
        last = first + per
        turned_ref[:, first:last] = x_ref[first:last, :].T
        q = x_ref[first:last, 0:HD]
        k = x_ref[0:last, HD : 2 * HD]
        v = x_ref[0:last, 2 * HD : 3 * HD]
        c = x_ref[first:last, 3 * HD : 4 * HD]
        c_turned = turned_ref[3 * HD : 4 * HD, first:last].astype(F32)
        near = turned_ref[4 * HD : 5 * HD, first:last].astype(F32)
        stat = turned_ref[STAT : STAT + 16, first:last].astype(F32)
        row_at, row_mid, row_far, place = codes(
            lax.broadcasted_iota(jnp.int32, (1, per), 1) + first
        )
        row_one = jnp.where(row_mid, row_at, -1)
        row_two = jnp.where(row_far, row_at, -1)
        three = stat[0:1] + stat[1:2] + stat[2:3]
        sums[0] = sums[0] + jnp.where(place == SUM_ROW, three, 0.0)
        gate = jnp.where(place == SUM_ROW, 0.0, three) + b0
        one = one_ref[0:last, :] <= row_one
        two = two_ref[0:last, :] <= row_two
        factor = jnp.where(one, e1, 0.0) + jnp.where(two, e2, 0.0)
        s = jnp.where(jnp.logical_or(one, two), dot(k, q, 1, 1) * scale, HIDDEN)
        top = jnp.maximum(jnp.max(s, axis=0, keepdims=True), gate)
        plain = jnp.exp(s - top)
        weight = plain * factor
        share = jnp.exp(gate - top)
        size = jnp.sum(weight, axis=0, keepdims=True) + share
        inverse = 1.0 / size
        total = top + jnp.log(size)
        out = dot(turned_ref[2 * HD : 3 * HD, 0:last], weight.astype(BF16))
        att = ((out + share * near) * inverse).astype(BF16).astype(F32)
        delta = jnp.sum(c_turned * att, axis=0, keepdims=True)
        near_delta = jnp.sum(c_turned * near, axis=0, keepdims=True)
        sums[0] = sums[0] + share * inverse * (near_delta - delta)
        slope = (dot(v, c, 1, 1) - delta) * inverse
        raw = plain * slope
        sums[1] = sums[1] + jnp.sum(jnp.where(one, raw, 0.0), axis=0, keepdims=True) * e1
        sums[2] = sums[2] + jnp.sum(jnp.where(two, raw, 0.0), axis=0, keepdims=True) * e2
        dscore = (raw * factor).astype(BF16)
        weight_low = (weight * inverse).astype(BF16)
        dk_ref[0:last, :] += dot(dscore, q)
        dv_ref[0:last, :] += dot(weight_low, c)
        dq = dot(turned_ref[HD : 2 * HD, 0:last], dscore)
        stats = stacked(three_parts(total) + three_parts(delta), 2 * HD, per)
        y_ref[first:last, 0 : 2 * HD] = jnp.concatenate([dq, att], axis=0).T.astype(BF16)
        y_ref[first:last, BACK_STAT : BACK_STAT + 2 * HD] = stats.T.astype(BF16)
    row = lax.broadcasted_iota(jnp.int32, (total_rows, HD), 0)
    place = row - jnp.right_shift(row * 1639, 16) * ROWS
    mine = lax.broadcasted_iota(jnp.int32, (total_rows, HD), 1) == column
    dk, dv = dk_ref[...], dv_ref[...]
    sums = [three_parts(jnp.sum(part, axis=1, keepdims=True)) for part in sums]
    for n in range(2):
        here = jnp.logical_and(mine, place == SUM_ROW + n)
        dk = jnp.where(here, sums[0][n], dk)
        dv = jnp.where(here, sums[1][n], dv)
        here = jnp.logical_and(mine, place == SUM_ROW + 2 + n)
        dk = jnp.where(here, sums[2][n], dk)
    y_ref[:, 2 * HD : 3 * HD] = dk.astype(BF16)
    y_ref[:, 3 * HD : 4 * HD] = dv.astype(BF16)


def bias_kernel(heads, y_ref, out_ref):
    tile = y_ref[0, ROWS - 8 : ROWS, 2 * HD : 4 * HD].astype(F32)
    for h in range(1, heads):
        tile = tile + y_ref[h * STRIDE, ROWS - 8 : ROWS, 2 * HD : 4 * HD].astype(F32)
    out_ref[...] = jnp.broadcast_to(tile[None], out_ref.shape)


def bias_sum_kernel(factor, x_ref, out_ref):
    count = out_ref.shape[1]
    tile = jnp.sum(x_ref[...], axis=0) * factor
    first = tile[4:5] + tile[5:6]
    out_ref[0:1, :] = first[:, 0:count]
    out_ref[1:2, :] = first[:, HD : HD + count]
    out_ref[2:3, :] = (tile[6:7] + tile[7:8])[:, 0:count]


def finish_kernel(
    mid_ref,
    far_ref,
    bias_ref,
    k_ref,
    v_ref,
    send_ref,
    y_ref,
    near_ref,
    dq_ref,
    dk_ref,
    dv_ref,
    att_out,
    dq_out,
    dk_out,
    dv_out,
):
    tok = k_ref.shape[2]
    heads = k_ref.shape[1] // HD
    scale = HD**-0.5
    place = lax.broadcasted_iota(jnp.int32, (ROWS, tok), 0)
    key_at = lax.broadcasted_iota(jnp.int32, (ROWS, tok), 1)
    for h in range(heads):
        mid, far = mid_ref[h], far_ref[h]
        own = slice(h * HD, (h + 1) * HD)
        k, v = k_ref[0, own, :], v_ref[0, own, :]
        block = h * STRIDE
        q = send_ref[block, :, 0:HD]
        c = send_ref[block, :, 3 * HD : 4 * HD]
        stat = y_ref[block, :, BACK_STAT : BACK_STAT + 8].astype(F32)
        total = stat[:, 0:1] + stat[:, 1:2] + stat[:, 2:3]
        delta = stat[:, 3:4] + stat[:, 4:5] + stat[:, 5:6]
        at, in_mid, in_far, _ = row_places(place, mid, far)
        used = jnp.logical_or(in_mid, in_far)
        s = dot(q, k) * scale + (bias_ref[0, h] - total)
        weight = jnp.exp(jnp.where(jnp.logical_and(used, key_at <= at), s, HIDDEN))
        dscore = (weight * (dot(c, v) - delta)).astype(BF16)
        weight = weight.astype(BF16)
        dq = dot(dscore, k, 1, 1) + y_ref[block, :, 0:HD].astype(F32)
        rest = y_ref[block, :, HD : 4 * HD]
        pick = jnp.where(jnp.logical_and(used, key_at == at), 1.0, 0.0).astype(BF16)
        dq = dot((dq * scale).astype(BF16), pick, 0, 0).astype(BF16)
        rest = dot(rest, pick, 0, 0)
        both = dilated(tok, mid, far)
        dq_out[0, own, :] = jnp.where(both, dq, (dq_ref[own, :] * scale).astype(BF16))
        att_out[0, own, :] = jnp.where(both, rest[0:HD].astype(BF16), near_ref[own, :])
        dk = dk_ref[own, :] + dot(q, dscore, 0, 0) + rest[HD : 2 * HD]
        dk_out[0, own, :] = (dk * scale).astype(BF16)
        dv = dv_ref[own, :] + dot(c, weight, 0, 0) + rest[2 * HD : 3 * HD]
        dv_out[0, own, :] = dv.astype(BF16)


def per_device(queries, keys, values, cotangent, level_bias, off_mid, off_far):
    tok, width = queries.shape[1:]
    heads = level_bias.shape[1]
    peers = lax.axis_size(GROUP)
    others = lax.axis_size(DP_SEQ)
    all_heads = heads * lax.axis_size(SEQ)
    smem = pl.BlockSpec(memory_space=pltpu.SMEM)
    vmem = pl.BlockSpec(memory_space=pltpu.VMEM)
    queries, keys, values, cotangent = (
        jnp.swapaxes(a, 1, 2) for a in (queries, keys, values, cotangent)
    )
    slab = (queries, keys, values, cotangent)
    shape = jax.ShapeDtypeStruct

    def call(kernel, name, in_specs, out_shape, flops, scratch=()):
        single = not isinstance(out_shape, list)
        return pl.pallas_call(
            kernel,
            name=name,
            in_specs=in_specs,
            out_specs=vmem if single else [vmem] * len(out_shape),
            out_shape=out_shape,
            scratch_shapes=list(scratch),
            compiler_params=pltpu.CompilerParams(vmem_limit_bytes=24 << 20),
            cost_estimate=pl.CostEstimate(
                flops=flops, transcendentals=0, bytes_accessed=1 << 20
            ),
        )

    send, stats, near = call(
        near_forward_kernel,
        "near_forward",
        [smem, smem] + [vmem] * 4,
        [
            shape((peers, ROWS, COLS), BF16),
            shape((16, tok), F32),
            shape((width, tok), BF16),
        ],
        200_000_000,
    )(off_mid, off_far, *slab)
    taken = lax.all_to_all(send, GROUP, 0, 0, tiled=True)
    near_grads = call(
        near_backward_kernel,
        "near_backward",
        [smem, smem] + [vmem] * 5,
        [shape((width, tok), F32)] * 3,
        400_000_000,
    )(off_mid, off_far, *slab, stats)
    taken, near_grads = lax.optimization_barrier((taken, near_grads))
    rows = peers * ROWS
    done = call(
        far_kernel,
        "mid_far",
        [smem, smem, smem, vmem],
        shape((rows, COLS), BF16),
        200_000_000,
        [
            pltpu.VMEM((COLS, rows), BF16),
            pltpu.VMEM((rows, 128), jnp.int32),
            pltpu.VMEM((rows, 128), jnp.int32),
            pltpu.VMEM((rows, HD), F32),
            pltpu.VMEM((rows, HD), F32),
        ],
    )(off_mid, off_far, level_bias, taken.reshape(rows, COLS))
    back = lax.all_to_all(done.reshape(peers, ROWS, COLS), GROUP, 0, 0, tiled=True)
    bias = call(
        functools.partial(bias_kernel, heads),
        "bias_rows",
        [vmem],
        shape((others, 8, 128), F32),
        1_000_000,
    )(back)
    bias = lax.all_to_all(bias, DP_SEQ, 0, 0, tiled=True)
    outs = call(
        finish_kernel,
        "finish",
        [smem] * 3 + [vmem] * 8,
        [shape((1, width, tok), BF16)] * 4,
        200_000_000,
    )(off_mid, off_far, level_bias, keys, values, send, back, near, *near_grads)
    factor = 1.0 / math.sqrt(lax.axis_size("dp") * peers * tok)
    bias_grad = call(
        functools.partial(bias_sum_kernel, factor),
        "bias_sum",
        [vmem],
        shape((3, all_heads), F32),
        1_000_000,
    )(bias)
    return (*(jnp.swapaxes(a, 1, 2) for a in outs), bias_grad)


def solution(mesh):
    finer = Mesh(
        mesh.devices.reshape(mesh.shape["dp"], 4, 4, 4, 2),
        ("dp", "group_0", "group_1", "seq_0", "seq_1"),
    )
    slab = P("dp", GROUP, SEQ)
    return jax.shard_map(
        per_device,
        mesh=finer,
        in_specs=(slab, slab, slab, slab, P(None, SEQ), P(SEQ), P(SEQ)),
        out_specs=(slab, slab, slab, slab, P()),
        check_vma=False,
    )
```
